32 devices in a mesh: grp: 2 (over x), seq: 4 (over y, core), head: 4 (over z).
Axes of the slice: x: 2, y: 2, z: 4, core: 2. Of those that a mesh axis runs over, the one named last changes fastest.
Arguments:
- q_latent: bfloat16 [8, 128, 512], P(('grp', 'seq'), 'head'), parts along dimension 0, may hold values from -6 to 6
- q_rope: bfloat16 [8, 128, 64], P(('grp', 'seq'), 'head'), parts along dimension 0, may hold values from -6 to 6
- cache_latent: bfloat16 [1152, 128, 512], P(('grp', 'seq', 'head')), parts along dimension 0, may hold values from -6 to 6
- cache_rope: bfloat16 [1152, 64, 128], P(('grp', 'seq', 'head')), parts along dimension 0, may hold values from -6 to 6
- page_table: int32 [8, 224], P(('grp', 'seq')), parts along dimension 0, may hold values from -1 to 575, as said below
- lengths: int32 [8], P(('grp', 'seq')), parts along dimension 0, may hold values from 1 to 28672, as said below
Outputs:
- attended: bfloat16 [8, 128, 512], P(('grp', 'seq'), 'head'), parts along dimension 0
The draws below stay inside these ranges and needn't reach their ends.
There are 2 independent parts, one for each index of `grp`. The reference program is written for one: setup_inputs(seed, part) draws one part's arguments, and reference() takes and returns one part's arrays. A program takes and returns all parts, laid end to end along the dimension named above; each array names one. Nothing has to cross between parts.
Inputs may be any that keep to these rules, and one draw needn't show every extreme that they name: `page_table`: row s holds the pool slots of the pages of sequence s in page order; entries from ceil(lengths[s] / 128) on are -1; no slot appears twice in the table. Slots d * 36 to (d + 1) * 36 - 1 belong to device d of seq+head (seq index first). One device holds at most 14 pages of one sequence; one sequence has exactly 14 pages on every device. Sequence s has ceil(lengths[s] / 128) pages; the sequence with 14 pages on every device has length 28672.
All inputs are finite; a program needn't handle non-finite values.
Results may differ from the reference program's by a relative error of at most 0.007.
Values may be sent and summed in bfloat16 or wider, within the bound.
A program may use at most 64 MiB of HBM per device.

```python
import jax
import jax.numpy as jnp
from jax import lax

HEADS = 128
LAT = 512
ROPE = 64
PAGE = 128
SLOTS = 36
SEQS = 4
NODES = 16
SLOTS_ALL = 576
SHARE = 7
MOST = 14
MAXP = 224


def pool_layout(key):
    key_list = jax.random.split(jax.random.fold_in(key, 23), 8)
    device_level = jax.random.randint(key_list[0], (NODES, 1), 1, 5)
    base_count = jax.random.randint(key_list[1], (NODES, SEQS), 0, SHARE + 1)
    page_counts = base_count * device_level // 4
    hot_seq = jax.random.randint(key_list[2], (), 0, SEQS)
    fuller = jax.random.randint(key_list[3], (), 0, NODES)
    seq_column = jnp.arange(SEQS, dtype=jnp.int32)[None, :]
    node_ids = jnp.arange(NODES, dtype=jnp.int32)[:, None]
    page_counts = jnp.where(node_ids == fuller, SHARE, page_counts)
    page_counts = jnp.where(seq_column == hot_seq, MOST, page_counts)
    within = jnp.arange(MOST, dtype=jnp.int32)
    used = within[None, None, :] < page_counts[:, :, None]
    flat_width = SEQS * MOST
    noise_one = jax.random.randint(key_list[4], (NODES, flat_width), 0, 2 ** 30 // flat_width)
    entry_ids = jnp.arange(flat_width, dtype=jnp.int32)[None, :]
    rank_keys = jnp.where(used.reshape(NODES, flat_width), noise_one * flat_width + entry_ids, 2 ** 30 + entry_ids)
    ranking = jnp.argsort(jnp.argsort(rank_keys, axis=1), axis=1)
    slot_noise = jax.random.randint(key_list[5], (NODES, SLOTS), 0, 2 ** 30 // SLOTS)
    slot_perm = jnp.argsort(slot_noise * SLOTS + jnp.arange(SLOTS, dtype=jnp.int32)[None, :], axis=1)
    local_slot = jnp.take_along_axis(slot_perm, jnp.minimum(ranking, SLOTS - 1), axis=1)
    global_slot = (node_ids * SLOTS + local_slot).reshape(NODES, SEQS, MOST)
    cand_slot = jnp.transpose(global_slot, (1, 0, 2)).reshape(SEQS, MAXP)
    cand_used = jnp.transpose(used, (1, 0, 2)).reshape(SEQS, MAXP)
    noise_two = jax.random.randint(key_list[6], (SEQS, MAXP), 0, 2 ** 30 // MAXP)
    spots = jnp.arange(MAXP, dtype=jnp.int32)[None, :]
    order_keys = jnp.where(cand_used, noise_two * MAXP + spots, 2 ** 30 + spots)
    picked = jnp.argsort(order_keys, axis=1)
    table = jnp.take_along_axis(cand_slot, picked, axis=1)
    page_total = jnp.sum(page_counts, axis=0)
    table = jnp.where(spots < page_total[:, None], table, -1)
    last_fill = jax.random.randint(key_list[7], (SEQS,), 1, PAGE + 1)
    last_fill = jnp.where(jnp.arange(SEQS, dtype=jnp.int32) == hot_seq, PAGE, last_fill)
    seq_lengths = (page_total - 1) * PAGE + last_fill
    return (table.astype(jnp.int32), seq_lengths.astype(jnp.int32))


def draw_page_table(key, part):
    return pool_layout(key)[0]


def draw_lengths(key, part):
    return pool_layout(key)[1]


def draw_q_latent(key, part):
    own_key = jax.random.fold_in(key, 31)
    values = jax.random.truncated_normal(own_key, -6.0, 6.0, (SEQS, HEADS, LAT), jnp.float32)
    return values.astype(jnp.bfloat16)


def draw_cache_latent(key, part):
    noise = jax.random.truncated_normal(jax.random.fold_in(key, 41), -6.0, 6.0, (SLOTS_ALL, PAGE, LAT), jnp.float32)
    values = noise
    return values.astype(jnp.bfloat16)


def block_levels(rng, extent, cuts, least, top_value):
    loudness, own = 1.0, jax.random.fold_in(rng, 6)
    for dim, parts in cuts:
        heights = jnp.exp(jax.random.uniform(jax.random.fold_in(own, dim), (parts,), jnp.float32, least / len(cuts), top_value / len(cuts)))
        loudness = loudness * jnp.repeat(heights, extent[dim] // parts).reshape([-1 if axis == dim else 1 for axis in range(len(extent))])
    return loudness


def centred(key, extent, spread, most, shards=(), kind=jnp.bfloat16):
    result = spread * jax.random.normal(key, extent, jnp.float32)
    if shards:
        result = result * block_levels(key, extent, shards, -0.22, 0.18)
    return jnp.clip(result, -most, most).astype(kind)


def setup_inputs(seed: int = 0, part: int = 0) -> dict:
    key_of = jax.random.split(jax.random.key(seed), 7)
    own_keys = jax.random.split(jax.random.fold_in(key_of[6], part), 7)
    return {
        "q_latent": draw_q_latent(jax.random.fold_in(jax.random.fold_in(key_of[6], part), 71), part),
        "q_rope": centred(own_keys[1], (SEQS, HEADS, ROPE), 1.0, 6.0, ((0, 4), (1, 4))),
        "cache_latent": draw_cache_latent(jax.random.fold_in(jax.random.fold_in(key_of[6], part), 71), part),
        "cache_rope": centred(own_keys[3], (SLOTS_ALL, ROPE, PAGE), 1.0, 6.0, ((0, 16),)),
        "page_table": draw_page_table(jax.random.fold_in(jax.random.fold_in(key_of[6], part), 71), part),
        "lengths": draw_lengths(jax.random.fold_in(jax.random.fold_in(key_of[6], part), 71), part),
    }


softmax_scale = 0.13528
floor_score = -1.0e30
page_block = 32


def one_sequence(query_lat, query_rot, table_row, length, cache_latent, cache_rope):
    page_len = cache_latent.shape[1]
    lat_width = cache_latent.shape[2]
    row_width = table_row.shape[0]
    padded_width = ((row_width + page_block - 1) // page_block) * page_block
    table_row = jnp.concatenate([table_row.astype(jnp.int32), jnp.full((padded_width - row_width,), -1, jnp.int32)])
    block_rows = table_row.reshape(padded_width // page_block, page_block)
    first_pages = jnp.arange(padded_width // page_block, dtype=jnp.int32) * page_block
    query_lat = query_lat.astype(jnp.float32)
    query_rot = query_rot.astype(jnp.float32)
    head_count = query_lat.shape[0]
    token_offset = jnp.arange(page_len, dtype=jnp.int32)
    block_pages = jnp.arange(page_block, dtype=jnp.int32)

    def block_scores(inputs):
        start_page, slot_ids = inputs

        def compute(operand):
            safe_ids = jnp.maximum(slot_ids, 0)
            latent = cache_latent[safe_ids].astype(jnp.float32)
            rotary = cache_rope[safe_ids].astype(jnp.float32)
            scores = jnp.einsum("hd,btd->hbt", query_lat, latent, precision=lax.Precision.HIGHEST)
            scores = scores + jnp.einsum("he,bet->hbt", query_rot, rotary, precision=lax.Precision.HIGHEST)
            position = (start_page + block_pages)[:, None] * page_len + token_offset[None, :]
            usable = (slot_ids[:, None] >= 0) & (position < length)
            return jnp.where(usable[None], scores * softmax_scale, floor_score).reshape(head_count, page_block * page_len)

        def skipped(operand):
            return jnp.full((head_count, page_block * page_len), floor_score, jnp.float32)

        return lax.cond(start_page * page_len < length, compute, skipped, 0)

    all_scores = lax.map(block_scores, (first_pages, block_rows))
    best_top = jnp.max(all_scores, axis=(0, 2))

    def block_mix(carry, inputs):
        start_page, slot_ids, scores = inputs

        def compute(operand):
            latent = cache_latent[jnp.maximum(slot_ids, 0)].reshape(page_block * page_len, lat_width)
            weight = jnp.exp(scores - best_top[:, None])
            total_part = jnp.sum(weight, axis=1)
            mixed_part = jnp.dot(weight.astype(jnp.bfloat16), latent, preferred_element_type=jnp.float32)
            return total_part, mixed_part

        def skipped(operand):
            return jnp.zeros((head_count,), jnp.float32), jnp.zeros((head_count, lat_width), jnp.float32)

        total_part, mixed_part = lax.cond(start_page * page_len < length, compute, skipped, 0)
        return (carry[0] + total_part, carry[1] + mixed_part), None

    start_carry = (jnp.zeros((head_count,), jnp.float32), jnp.zeros((head_count, lat_width), jnp.float32))
    (total_sum, mixed_sum), unused = lax.scan(block_mix, start_carry, (first_pages, block_rows, all_scores))
    return (mixed_sum / total_sum[:, None]).astype(jnp.bfloat16)


def reference(q_latent, q_rope, cache_latent, cache_rope, page_table, lengths):
    def per_sequence(inputs):
        query_lat, query_rot, table_row, length = inputs
        return one_sequence(query_lat, query_rot, table_row, length, cache_latent, cache_rope)

    return lax.map(per_sequence, (q_latent, q_rope, page_table, lengths))
```

```python
import functools

import jax
import jax.numpy as jnp
from jax import lax
from jax.experimental import pallas as pl
from jax.experimental.pallas import tpu as pltpu
from jax.sharding import PartitionSpec as P

MESH = pl.DeviceIdType.MESH
softmax_scale = 0.13528
floor_score = -1e30
F32 = jnp.float32
BF16 = jnp.bfloat16


def swapped(index, by):
    out, bit = index, 1
    while bit <= by:
        if by & bit:
            out = out + bit - 2 * bit * ((index // bit) % 2)
        bit *= 2
    return out


def kernel(
    n_s, n_h, window,
    ql, qr, kc, kr, tab, lens, out,
    kc_v, kr_v, ql_all, qr_all, tab_all, len_all, plan_v, plan_s, sc, acc, acc_m, acc_l,
    send_c, recv_c, send_y, recv_y, send_z, recv_z,
    cache_sem, plan_sem, tab_ss, tab_rs, q_ss, q_rs, c_ss, c_rs, y_ss, y_rs, z_ss, z_rs,
):
    s, h = lax.axis_index("seq"), lax.axis_index("head")
    y_count = n_s // 2
    slots, page, lat = kc.shape
    rows = ql.shape[1]
    heads = n_h * rows
    width = tab.shape[1]

    cache_copies = [
        pltpu.make_async_copy(kc, kc_v, cache_sem.at[0]),
        pltpu.make_async_copy(kr, kr_v, cache_sem.at[1]),
    ]
    for copy in cache_copies:
        copy.start()

    barrier = pltpu.get_barrier_semaphore()
    for d in range(1, n_s):
        pl.semaphore_signal(barrier, inc=1, device_id={"seq": swapped(s, d)}, device_id_type=MESH)
    for d in range(1, n_h):
        pl.semaphore_signal(barrier, inc=1, device_id={"head": swapped(h, d)}, device_id_type=MESH)
    pl.semaphore_wait(barrier, n_s + n_h - 2)

    sends = []

    def remote(src, dst, ss, rs, target):
        copy = pltpu.make_async_remote_copy(
            src_ref=src, dst_ref=dst, send_sem=ss, recv_sem=rs, device_id=target, device_id_type=MESH
        )
        copy.start()
        sends.append(copy)

    for d in range(1, n_s):
        target = {"seq": swapped(s, d)}
        remote(tab, tab_all.at[s], tab_ss.at[0, d], tab_rs.at[0, s], target)
        remote(lens, len_all.at[s], tab_ss.at[1, d], tab_rs.at[1, s], target)

    send_at = [0]

    def push(lat_src, rot_src, seq_slot, head_slot, target):
        i = send_at[0]
        send_at[0] += 1
        remote(lat_src, ql_all.at[seq_slot, head_slot], q_ss.at[0, i], q_rs.at[0, seq_slot, head_slot], target)
        remote(rot_src, qr_all.at[seq_slot, head_slot], q_ss.at[1, i], q_rs.at[1, seq_slot, head_slot], target)

    def landed(seq_slot, head_slot):
        for i, ref in enumerate((ql_all, qr_all)):
            at = ref.at[seq_slot, head_slot]
            pltpu.make_async_copy(at, at, q_rs.at[i, seq_slot, head_slot]).wait()

    for d in range(n_h - 1, 0, -1):
        push(ql.at[0], qr.at[0], s, h, {"head": swapped(h, d)})
    for k in range(1, y_count):
        push(ql.at[0], qr.at[0], s, h, {"seq": swapped(s, 2 * k)})
    push(ql.at[0], qr.at[0], s, h, {"seq": swapped(s, 1)})
    ql_all[s, h] = ql[0]
    qr_all[s, h] = qr[0]
    tab_all[s] = tab[...]
    len_all[s] = lens[...]

    for d in range(1, n_s):
        other = swapped(s, d)
        for i, ref in enumerate((tab_all, len_all)):
            at = ref.at[other]
            pltpu.make_async_copy(at, at, tab_rs.at[i, other]).wait()
    tables = tab_all[...].reshape(n_s, width)
    all_lens = len_all[...].reshape(n_s, 128)[:, :1]
    local = tables - (s * n_h + h) * slots
    hit = (local >= 0) & (local < slots) & (tables >= 0)
    before = lax.broadcasted_iota(jnp.int32, (width, width), 0) < lax.broadcasted_iota(jnp.int32, (width, width), 1)
    rank = jnp.dot(
        hit.astype(F32).astype(BF16), before.astype(F32).astype(BF16), preferred_element_type=F32
    ).astype(jnp.int32)
    page_no = lax.broadcasted_iota(jnp.int32, (n_s, width), 1)
    limit = jnp.clip(all_lens - page_no * page, 0, page)
    lane = lax.broadcasted_iota(jnp.int32, (n_s, 128), 1)
    slot_plan = jnp.zeros((n_s, 128), jnp.int32)
    limit_plan = jnp.zeros((n_s, 128), jnp.int32)
    for j in range(window):
        chosen = hit & (rank == j)
        slot_j = jnp.sum(jnp.where(chosen, local, 0), axis=1, keepdims=True)
        limit_j = jnp.sum(jnp.where(chosen, limit, 0), axis=1, keepdims=True)
        slot_plan = jnp.where(lane == j, slot_j, slot_plan)
        limit_plan = jnp.where(lane == j, limit_j, limit_plan)
    plan_v[0] = slot_plan
    plan_v[1] = limit_plan

    for d in range(1, n_h):
        g = swapped(h, d)
        landed(s, g)
        for k in range(1, y_count):
            push(ql_all.at[s, g], qr_all.at[s, g], s, g, {"seq": swapped(s, 2 * k)})
        push(ql_all.at[s, g], qr_all.at[s, g], s, g, {"seq": swapped(s, 1)})

    plan_copy = pltpu.make_async_copy(plan_v, plan_s, plan_sem.at[0])
    plan_copy.start()
    plan_copy.wait()
    for copy in cache_copies:
        copy.wait()

    group = 2 if window % 2 == 0 else 1
    steps = window // group
    span = group * page
    tokens = lax.broadcasted_iota(jnp.int32, (heads, page), 1)

    def attend(seq_slot):
        lat_q = ql_all[seq_slot].reshape(heads, lat)
        rot_q = qr_all[seq_slot].reshape(heads, qr.shape[2])
        best = None
        for p in range(steps):
            held = [plan_s[0, seq_slot, p * group + i] for i in range(group)]
            keys = jnp.concatenate([kc_v[i] for i in held], axis=0)
            rot = jnp.concatenate([kr_v[i] for i in held], axis=1)
            scores = lax.dot_general(lat_q, keys, (((1,), (1,)), ((), ())), preferred_element_type=F32)
            scores = scores + jnp.dot(rot_q, rot, preferred_element_type=F32)
            live = jnp.concatenate(
                [tokens < plan_s[1, seq_slot, p * group + i] for i in range(group)], axis=1
            )
            scores = jnp.where(live, scores * softmax_scale, floor_score)
            sc[p] = scores
            best = scores if best is None else jnp.maximum(best, scores)
        top = jnp.max(best, axis=1, keepdims=True).astype(BF16).astype(F32)
        shift = jnp.where(top > 0.1 * floor_score, top, 0.0)
        total = None
        for p in range(steps):
            held = [plan_s[0, seq_slot, p * group + i] for i in range(group)]
            keys = jnp.concatenate([kc_v[i] for i in held], axis=0)
            weight = jnp.exp(sc[p] - shift)
            total = weight if total is None else total + weight
            part = jnp.dot(weight.astype(BF16), keys, preferred_element_type=F32)
            if p == 0:
                acc[...] = part
            else:
                acc[...] += part
        return top, jnp.sum(total, axis=1, keepdims=True)

    def packed(mixed, top, total):
        high = total.astype(BF16)
        low = (total - high.astype(F32)).astype(BF16)
        at = lax.broadcasted_iota(jnp.int32, (mixed.shape[0], 128), 1)
        stats = jnp.where(at == 0, top, jnp.where(at == 1, high.astype(F32), low.astype(F32)))
        return jnp.concatenate([mixed.astype(BF16), stats.astype(BF16)], axis=1)

    def unpacked(block):
        mixed = block[:, :lat].astype(F32)
        stats = block[:, lat:].astype(F32)
        return mixed, stats[:, 0:1], stats[:, 1:2] + stats[:, 2:3]

    def merged(states):
        top = functools.reduce(jnp.maximum, [state[1] for state in states])
        mixed, total = 0.0, 0.0
        for part_mixed, part_top, part_total in states:
            factor = jnp.exp(part_top - top)
            mixed = mixed + factor * part_mixed
            total = total + factor * part_total
        return mixed, top, total

    def own_part(k):
        top, total = attend(swapped(s, 2 * k))
        acc_m[k] = acc[...]
        acc_l[0, k] = jnp.broadcast_to(top, (heads, 128))
        acc_l[1, k] = jnp.broadcast_to(total, (heads, 128))

    def partner_part(k):
        top, total = attend(swapped(s, 2 * k + 1))
        send_c[k] = packed(acc[...], top, total)
        remote(send_c.at[k], recv_c.at[k], c_ss.at[k], c_rs.at[k], {"seq": swapped(s, 1)})

    own_part(0)
    for k in range(1, y_count):
        other = swapped(s, 2 * k)
        for d in range(n_h):
            g = swapped(h, d)
            landed(other, g)
            push(ql_all.at[other, g], qr_all.at[other, g], other, g, {"seq": swapped(s, 1)})
    for k in range(y_count):
        other = swapped(s, 2 * k + 1)
        for d in range(n_h):
            landed(other, swapped(h, d))
        partner_part(k)
        if k > 0:
            own_part(k)

    def group_state(k, g):
        at = pl.ds(pl.multiple_of(g * rows, rows), rows)
        mine = (acc_m[k, at, :], acc_l[0, k, at, :][:, :1], acc_l[1, k, at, :][:, :1])
        theirs = unpacked(recv_c[k, at, :])
        return [mine, theirs]

    def wait_block(ref, sem):
        pltpu.make_async_copy(ref, ref, sem).wait()

    order = list(range(n_h - 1, -1, -1))
    for k in range(1, y_count):
        wait_block(recv_c.at[k], c_rs.at[k])
        for d in order:
            g = swapped(h, d)
            send_y[k - 1, d] = packed(*merged(group_state(k, g)))
            remote(
                send_y.at[k - 1, d], recv_y.at[k - 1, d], y_ss.at[k - 1, d], y_rs.at[k - 1, d],
                {"seq": swapped(s, 2 * k)},
            )
    wait_block(recv_c.at[0], c_rs.at[0])
    final = None
    for d in order:
        states = group_state(0, swapped(h, d))
        for k in range(1, y_count):
            wait_block(recv_y.at[k - 1, d], y_rs.at[k - 1, d])
            states.append(unpacked(recv_y[k - 1, d]))
        state = merged(states)
        if d > 0:
            send_z[d - 1] = packed(*state)
            remote(
                send_z.at[d - 1], recv_z.at[d - 1], z_ss.at[d - 1], z_rs.at[d - 1],
                {"head": swapped(h, d)},
            )
        else:
            final = [state]
    for d in range(1, n_h):
        wait_block(recv_z.at[d - 1], z_rs.at[d - 1])
        final.append(unpacked(recv_z[d - 1]))
    mixed, _, total = merged(final)
    out[0] = (mixed / total).astype(BF16)
    for copy in sends:
        copy.wait_send()


def solution(mesh):
    n_s, n_h = mesh.shape["seq"], mesh.shape["head"]

    def on_device(q_latent, q_rope, cache_latent, cache_rope, page_table, lengths):
        slots, page, lat = cache_latent.shape
        rot = cache_rope.shape[1]
        rows = q_latent.shape[1]
        heads = rows * n_h
        width = page_table.shape[1]
        window = width // (n_s * n_h)
        y_count = n_s // 2
        group = 2 if window % 2 == 0 else 1
        pack = lat + 128
        dma = pltpu.SemaphoreType.DMA
        others = max(y_count - 1, 1)
        pushes = (n_h - 1) + n_h * y_count + n_h * (y_count - 1)
        vmem = pl.BlockSpec(memory_space=pltpu.VMEM)
        anyspace = pl.BlockSpec(memory_space=pl.ANY)
        padded = jnp.broadcast_to(lengths.reshape(1, 1), (1, 128))
        return pl.pallas_call(
            functools.partial(kernel, n_s, n_h, window),
            out_shape=jax.ShapeDtypeStruct((1, rows, lat), BF16),
            in_specs=[vmem, vmem, anyspace, anyspace, vmem, vmem],
            out_specs=vmem,
            scratch_shapes=[
                pltpu.VMEM((slots, page, lat), BF16),
                pltpu.VMEM((slots, rot, page), BF16),
                pltpu.VMEM((n_s, n_h, rows, lat), BF16),
                pltpu.VMEM((n_s, n_h, rows, rot), BF16),
                pltpu.VMEM((n_s, 1, width), jnp.int32),
                pltpu.VMEM((n_s, 1, 128), jnp.int32),
                pltpu.VMEM((2, n_s, 128), jnp.int32),
                pltpu.SMEM((2, n_s, 128), jnp.int32),
                pltpu.VMEM((window // group, heads, group * page), F32),
                pltpu.VMEM((heads, lat), F32),
                pltpu.VMEM((y_count, heads, lat), F32),
                pltpu.VMEM((2, y_count, heads, 128), F32),
                pltpu.VMEM((y_count, heads, pack), BF16),
                pltpu.VMEM((y_count, heads, pack), BF16),
                pltpu.VMEM((others, n_h, rows, pack), BF16),
                pltpu.VMEM((others, n_h, rows, pack), BF16),
                pltpu.VMEM((n_h - 1, rows, pack), BF16),
                pltpu.VMEM((n_h - 1, rows, pack), BF16),
                dma((2,)),
                dma((1,)),
                dma((2, n_s)),
                dma((2, n_s)),
                dma((2, pushes)),
                dma((2, n_s, n_h)),
                dma((y_count,)),
                dma((y_count,)),
                dma((others, n_h)),
                dma((others, n_h)),
                dma((n_h - 1,)),
                dma((n_h - 1,)),
            ],
            compiler_params=pltpu.CompilerParams(
                collective_id=0, has_side_effects=True, vmem_limit_bytes=48 * 1024 * 1024
            ),
        )(q_latent, q_rope, cache_latent, cache_rope, page_table, padded)

    placed = (
        P(("grp", "seq"), "head", None),
        P(("grp", "seq"), "head", None),
        P(("grp", "seq", "head"), None, None),
        P(("grp", "seq", "head"), None, None),
        P(("grp", "seq"), None),
        P(("grp", "seq")),
    )
    return jax.shard_map(
        on_device,
        mesh=mesh,
        in_specs=placed,
        out_specs=P(("grp", "seq"), "head", None),
        check_vma=False,
    )
```

```python
import functools

import jax
import jax.numpy as jnp
from jax import lax
from jax.experimental import pallas as pl
from jax.experimental.pallas import tpu as pltpu
from jax.sharding import PartitionSpec as P

MESH = pl.DeviceIdType.MESH
softmax_scale = 0.13528
floor_score = -1e30
F32 = jnp.float32
BF16 = jnp.bfloat16


def swapped(index, by):
    out, bit = index, 1
    while bit <= by:
        if by & bit:
            out = out + bit - 2 * bit * ((index // bit) % 2)
        bit *= 2
    return out


def kernel(
    n_s, n_h, window,
    ql, qr, kc, kr, tab, lens, out,
    kc_v, kr_v, ql_all, qr_all, tab_all, len_all, plan_v, plan_s, sc, weights, acc, acc_m, acc_l,
    send_c, recv_c, send_y, recv_y, send_z, recv_z,
    cache_sem, own_sem, plan_sem, tab_ss, tab_rs, q_ss, q_rs, c_ss, c_rs, y_ss, y_rs, z_ss, z_rs,
):
    s, h = lax.axis_index("seq"), lax.axis_index("head")
    y_count = n_s // 2
    slots, page, lat = kc.shape
    rows = ql.shape[1]
    heads = n_h * rows
    width = tab.shape[1]

    cache_copies = [
        pltpu.make_async_copy(kc, kc_v, cache_sem.at[0]),
        pltpu.make_async_copy(kr, kr_v, cache_sem.at[1]),
    ]
    own_copies = [
        pltpu.make_async_copy(tab, tab_all.at[s], own_sem.at[0]),
        pltpu.make_async_copy(ql.at[0], ql_all.at[s, h], own_sem.at[1]),
        pltpu.make_async_copy(qr.at[0], qr_all.at[s, h], own_sem.at[2]),
    ]
    for copy in own_copies + cache_copies:
        copy.start()

    barrier = pltpu.get_barrier_semaphore()
    for d in range(1, n_s):
        pl.semaphore_signal(barrier, inc=1, device_id={"seq": swapped(s, d)}, device_id_type=MESH)
    for d in range(1, n_h):
        pl.semaphore_signal(barrier, inc=1, device_id={"head": swapped(h, d)}, device_id_type=MESH)
    len_all[s] = lens[...]
    for copy in own_copies:
        copy.wait()
    pl.semaphore_wait(barrier, n_s + n_h - 2)

    sends = []

    def remote(src, dst, ss, rs, target):
        copy = pltpu.make_async_remote_copy(
            src_ref=src, dst_ref=dst, send_sem=ss, recv_sem=rs, device_id=target, device_id_type=MESH
        )
        copy.start()
        sends.append(copy)

    for d in range(1, n_s):
        target = {"seq": swapped(s, d)}
        remote(tab_all.at[s], tab_all.at[s], tab_ss.at[0, d], tab_rs.at[0, s], target)
        remote(lens, len_all.at[s], tab_ss.at[1, d], tab_rs.at[1, s], target)

    send_at = [0]

    def push(lat_src, rot_src, seq_slot, head_slot, target):
        i = send_at[0]
        send_at[0] += 1
        remote(lat_src, ql_all.at[seq_slot, head_slot], q_ss.at[0, i], q_rs.at[0, seq_slot, head_slot], target)
        remote(rot_src, qr_all.at[seq_slot, head_slot], q_ss.at[1, i], q_rs.at[1, seq_slot, head_slot], target)

    def landed(seq_slot, head_slot):
        for i, ref in enumerate((ql_all, qr_all)):
            at = ref.at[seq_slot, head_slot]
            pltpu.make_async_copy(at, at, q_rs.at[i, seq_slot, head_slot]).wait()

    for d in range(n_h - 1, 0, -1):
        push(ql_all.at[s, h], qr_all.at[s, h], s, h, {"head": swapped(h, d)})
    for k in range(1, y_count):
        push(ql_all.at[s, h], qr_all.at[s, h], s, h, {"seq": swapped(s, 2 * k)})
    push(ql_all.at[s, h], qr_all.at[s, h], s, h, {"seq": swapped(s, 1)})

    for d in range(1, n_s):
        other = swapped(s, d)
        for i, ref in enumerate((tab_all, len_all)):
            at = ref.at[other]
            pltpu.make_async_copy(at, at, tab_rs.at[i, other]).wait()
    tables = tab_all[...].reshape(n_s, width)
    all_lens = len_all[...].reshape(n_s, 128)[:, :1]
    local = tables - (s * n_h + h) * slots
    hit = (local >= 0) & (local < slots) & (tables >= 0)
    before = lax.broadcasted_iota(jnp.int32, (width, width), 0) < lax.broadcasted_iota(jnp.int32, (width, width), 1)
    rank = jnp.dot(
        hit.astype(F32).astype(BF16), before.astype(F32).astype(BF16), preferred_element_type=F32
    ).astype(jnp.int32)
    page_no = lax.broadcasted_iota(jnp.int32, (n_s, width), 1)
    limit = jnp.clip(all_lens - page_no * page, 0, page)
    lane = lax.broadcasted_iota(jnp.int32, (n_s, 128), 1)
    slot_plan = jnp.zeros((n_s, 128), jnp.int32)
    limit_plan = jnp.zeros((n_s, 128), jnp.int32)
    for j in range(window):
        chosen = hit & (rank == j)
        slot_j = jnp.sum(jnp.where(chosen, local, 0), axis=1, keepdims=True)
        limit_j = jnp.sum(jnp.where(chosen, limit, 0), axis=1, keepdims=True)
        slot_plan = jnp.where(lane == j, slot_j, slot_plan)
        limit_plan = jnp.where(lane == j, limit_j, limit_plan)
    plan_v[0] = slot_plan
    plan_v[1] = limit_plan

    for d in range(1, n_h):
        g = swapped(h, d)
        landed(s, g)
        for k in range(1, y_count):
            push(ql_all.at[s, g], qr_all.at[s, g], s, g, {"seq": swapped(s, 2 * k)})
        push(ql_all.at[s, g], qr_all.at[s, g], s, g, {"seq": swapped(s, 1)})

    plan_copy = pltpu.make_async_copy(plan_v, plan_s, plan_sem.at[0])
    plan_copy.start()
    plan_copy.wait()
    for copy in cache_copies:
        copy.wait()

    group = 2 if window % 2 == 0 else 1
    steps = window // group
    mix = window
    span = group * page
    tokens = lax.broadcasted_iota(jnp.int32, (heads, page), 1)

    def attend(seq_slot):
        lat_q = ql_all[seq_slot].reshape(heads, lat)
        rot_q = qr_all[seq_slot].reshape(heads, qr.shape[2])
        best = None
        for p in range(steps):
            held = [plan_s[0, seq_slot, p * group + i] for i in range(group)]
            keys = jnp.concatenate([kc_v[i] for i in held], axis=0)
            rot = jnp.concatenate([kr_v[i] for i in held], axis=1)
            scores = lax.dot_general(lat_q, keys, (((1,), (1,)), ((), ())), preferred_element_type=F32)
            scores = scores + jnp.dot(rot_q, rot, preferred_element_type=F32)
            live = jnp.concatenate(
                [tokens < plan_s[1, seq_slot, p * group + i] for i in range(group)], axis=1
            )
            scores = jnp.where(live, scores * softmax_scale, floor_score)
            sc[p] = scores
            best = scores if best is None else jnp.maximum(best, scores)
        top = jnp.max(best, axis=1, keepdims=True).astype(BF16).astype(F32)
        shift = jnp.where(top > 0.1 * floor_score, top, 0.0)
        total = None
        for p in range(steps):
            weight = jnp.exp(sc[p] - shift)
            total = weight if total is None else total + weight
            weights[:, p * span : (p + 1) * span] = weight.astype(BF16)
        for p in range(0, window, mix):
            keys = jnp.concatenate([kc_v[plan_s[0, seq_slot, p + i]] for i in range(mix)], axis=0)
            part = jnp.dot(weights[:, p * page : (p + mix) * page], keys, preferred_element_type=F32)
            if p == 0:
                acc[...] = part
            else:
                acc[...] += part
        return top, jnp.sum(total, axis=1, keepdims=True)

    def packed(mixed, top, total):
        high = total.astype(BF16)
        low = (total - high.astype(F32)).astype(BF16)
        at = lax.broadcasted_iota(jnp.int32, (mixed.shape[0], 128), 1)
        stats = jnp.where(at == 0, top, jnp.where(at == 1, high.astype(F32), low.astype(F32)))
        return jnp.concatenate([mixed.astype(BF16), stats.astype(BF16)], axis=1)

    def unpacked(block):
        mixed = block[:, :lat].astype(F32)
        stats = block[:, lat:].astype(F32)
        return mixed, stats[:, 0:1], stats[:, 1:2] + stats[:, 2:3]

    def merged(states):
        top = functools.reduce(jnp.maximum, [state[1] for state in states])
        mixed, total = 0.0, 0.0
        for part_mixed, part_top, part_total in states:
            factor = jnp.exp(part_top - top)
            mixed = mixed + factor * part_mixed
            total = total + factor * part_total
        return mixed, top, total

    def own_part(k):
        top, total = attend(swapped(s, 2 * k))
        acc_m[k] = acc[...]
        acc_l[0, k] = jnp.broadcast_to(top, (heads, 128))
        acc_l[1, k] = jnp.broadcast_to(total, (heads, 128))

    def partner_part(k):
        top, total = attend(swapped(s, 2 * k + 1))
        send_c[k] = packed(acc[...], top, total)
        remote(send_c.at[k], recv_c.at[k], c_ss.at[k], c_rs.at[k], {"seq": swapped(s, 1)})

    own_part(0)
    for d in range(n_h):
        landed(swapped(s, 1), swapped(h, d))
    partner_part(0)
    for k in range(1, y_count):
        other = swapped(s, 2 * k)
        for d in range(n_h):
            g = swapped(h, d)
            landed(other, g)
            push(ql_all.at[other, g], qr_all.at[other, g], other, g, {"seq": swapped(s, 1)})
    for k in range(1, y_count):
        own_part(k)
        other = swapped(s, 2 * k + 1)
        for d in range(n_h):
            landed(other, swapped(h, d))
        partner_part(k)

    def group_state(k, g):
        at = pl.ds(pl.multiple_of(g * rows, rows), rows)
        mine = (acc_m[k, at, :], acc_l[0, k, at, :][:, :1], acc_l[1, k, at, :][:, :1])
        theirs = unpacked(recv_c[k, at, :])
        return [mine, theirs]

    def wait_block(ref, sem):
        pltpu.make_async_copy(ref, ref, sem).wait()

    order = list(range(n_h - 1, -1, -1))
    for k in range(1, y_count):
        wait_block(recv_c.at[k], c_rs.at[k])
        for d in order:
            g = swapped(h, d)
            send_y[k - 1, d] = packed(*merged(group_state(k, g)))
            remote(
                send_y.at[k - 1, d], recv_y.at[k - 1, d], y_ss.at[k - 1, d], y_rs.at[k - 1, d],
                {"seq": swapped(s, 2 * k)},
            )
    wait_block(recv_c.at[0], c_rs.at[0])
    final = None
    for d in order:
        states = group_state(0, swapped(h, d))
        for k in range(1, y_count):
            wait_block(recv_y.at[k - 1, d], y_rs.at[k - 1, d])
            states.append(unpacked(recv_y[k - 1, d]))
        state = merged(states)
        if d > 0:
            send_z[d - 1] = packed(*state)
            remote(
                send_z.at[d - 1], recv_z.at[d - 1], z_ss.at[d - 1], z_rs.at[d - 1],
                {"head": swapped(h, d)},
            )
        else:
            final = [state]
    for d in range(1, n_h):
        wait_block(recv_z.at[d - 1], z_rs.at[d - 1])
        final.append(unpacked(recv_z[d - 1]))
    mixed, _, total = merged(final)
    out[0] = (mixed / total).astype(BF16)
    for copy in sends:
        copy.wait_send()


def solution(mesh):
    n_s, n_h = mesh.shape["seq"], mesh.shape["head"]

    def on_device(q_latent, q_rope, cache_latent, cache_rope, page_table, lengths):
        slots, page, lat = cache_latent.shape
        rot = cache_rope.shape[1]
        rows = q_latent.shape[1]
        heads = rows * n_h
        width = page_table.shape[1]
        window = width // (n_s * n_h)
        y_count = n_s // 2
        group = 2 if window % 2 == 0 else 1
        pack = lat + 128
        dma = pltpu.SemaphoreType.DMA
        others = max(y_count - 1, 1)
        pushes = (n_h - 1) + n_h * y_count + n_h * (y_count - 1)
        vmem = pl.BlockSpec(memory_space=pltpu.VMEM)
        hbm = pl.BlockSpec(memory_space=pltpu.HBM)
        padded = jnp.broadcast_to(lengths.reshape(1, 1), (1, 128))
        return pl.pallas_call(
            functools.partial(kernel, n_s, n_h, window),
            out_shape=jax.ShapeDtypeStruct((1, rows, lat), BF16),
            in_specs=[hbm, hbm, hbm, hbm, hbm, vmem],
            out_specs=vmem,
            scratch_shapes=[
                pltpu.VMEM((slots, page, lat), BF16),
                pltpu.VMEM((slots, rot, page), BF16),
                pltpu.VMEM((n_s, n_h, rows, lat), BF16),
                pltpu.VMEM((n_s, n_h, rows, rot), BF16),
                pltpu.VMEM((n_s, 1, width), jnp.int32),
                pltpu.VMEM((n_s, 1, 128), jnp.int32),
                pltpu.VMEM((2, n_s, 128), jnp.int32),
                pltpu.SMEM((2, n_s, 128), jnp.int32),
                pltpu.VMEM((window // group, heads, group * page), F32),
                pltpu.VMEM((heads, window * page), BF16),
                pltpu.VMEM((heads, lat), F32),
                pltpu.VMEM((y_count, heads, lat), F32),
                pltpu.VMEM((2, y_count, heads, 128), F32),
                pltpu.VMEM((y_count, heads, pack), BF16),
                pltpu.VMEM((y_count, heads, pack), BF16),
                pltpu.VMEM((others, n_h, rows, pack), BF16),
                pltpu.VMEM((others, n_h, rows, pack), BF16),
                pltpu.VMEM((n_h - 1, rows, pack), BF16),
                pltpu.VMEM((n_h - 1, rows, pack), BF16),
                dma((2,)),
                dma((3,)),
                dma((1,)),
                dma((2, n_s)),
                dma((2, n_s)),
                dma((2, pushes)),
                dma((2, n_s, n_h)),
                dma((y_count,)),
                dma((y_count,)),
                dma((others, n_h)),
                dma((others, n_h)),
                dma((n_h - 1,)),
                dma((n_h - 1,)),
            ],
            compiler_params=pltpu.CompilerParams(
                collective_id=0, has_side_effects=True, vmem_limit_bytes=67_043_328
            ),
        )(q_latent, q_rope, cache_latent, cache_rope, page_table, padded)

    placed = (
        P(("grp", "seq"), "head", None),
        P(("grp", "seq"), "head", None),
        P(("grp", "seq", "head"), None, None),
        P(("grp", "seq", "head"), None, None),
        P(("grp", "seq"), None),
        P(("grp", "seq")),
    )
    return jax.shard_map(
        on_device,
        mesh=mesh,
        in_specs=placed,
        out_specs=P(("grp", "seq"), "head", None),
        check_vma=False,
    )
```
